512 devices in a mesh: ctx: 64 (over z, y_hi, core), req: 8 (over y_lo, x).
Axes of the slice: x: 4, y: 4 (y_hi: 2, y_lo: 2; y = y_hi * 2 + y_lo), z: 16, core: 2. Of those that a mesh axis runs over, the one named last changes fastest.
Arguments:
- hidden: bfloat16 [1024, 5120], P('req'), parts along dimension 0, may hold values from -6 to 6
- w_query: bfloat16 [5120, 8192], P(None, 'ctx'), may hold values from -0.078125 to 0.078125
- key_projection_weight: bfloat16 [5120, 1024], P(None, 'ctx'), may hold values from -0.078125 to 0.078125
- value_projection_weight: bfloat16 [5120, 1024], P(None, 'ctx'), may hold values from -0.078125 to 0.078125
- query_gain: float32 [128], replicated, may hold values from 0.5 to 1.5
- key_gain: float32 [128], replicated, may hold values from 4 to 8
- stored_cache_keys: bfloat16 [65536, 1024], P(('req', 'ctx')), parts along dimension 0, may hold values from -100 to 100
- stored_cache_values: bfloat16 [65536, 1024], P(('req', 'ctx')), parts along dimension 0, may hold values from -8 to 8
- cache_length: int32 [8], P('req'), parts along dimension 0, may hold values from 4096 to 8192
- first_position: int32 [8], P('req'), parts along dimension 0, may hold values from 0 to 4095
Outputs:
- attended: bfloat16 [1024, 8192], P('req', 'ctx'), parts along dimension 0
The draws below stay inside these ranges and needn't reach their ends.
There are 8 independent parts, one for each index of `req`. The reference program is written for one: setup_inputs(seed, part) draws one part's arguments, and reference() takes and returns one part's arrays. A program takes and returns all parts, laid end to end along the dimension named above; an argument that names none is the same for every part. Nothing has to cross between parts.
All inputs are finite; a program needn't handle non-finite values.
Results may differ from the reference program's by a relative error of at most 0.013.
The reference program's roundings to bfloat16 on the way count: a program that leaves them out, or rounds other values in their place, can miss the bound.
Values may be sent and summed in bfloat16 or wider, within the bound.
No kernel may reach another device: no remote copies, remote signals or barrier semaphores. Data moves between devices by JAX's collectives and lax.ppermute only.
A program may use at most 128 MiB of HBM per device.

```python
import math
import jax
import jax.numpy as jnp
from jax import lax

MODEL_WIDTH = 5120
QUERY_HEADS = 64
KEY_VALUE_HEADS = 8
HEAD_SIZE = 128
NEW = 128
CACHE_SLOTS = 8192


def draw_stored_cache_keys(key, part):
    rotary_base = jax.random.normal(jax.random.fold_in(key, 11), (CACHE_SLOTS, KEY_VALUE_HEADS * HEAD_SIZE), jnp.float32) * 2.5
    return jnp.clip(rotary_base, -100.0, 100.0).astype(jnp.bfloat16)


def level_of(stream_key, extent, shards, low, high):
    def one(axis_at, shards_of):
        heights = jax.random.uniform(jax.random.fold_in(jax.random.fold_in(stream_key, 6), axis_at), (shards_of,), jnp.float32, low / len(shards), high / len(shards))
        return jnp.repeat(jnp.exp(heights), extent[axis_at] // shards_of).reshape((-1,) + (1,) * (len(extent) - axis_at - 1))

    factor_of = one(*shards[0])
    for cut in shards[1:]:
        factor_of = factor_of * one(*cut)
    return factor_of


def centred(rng, shape, scale, limit, shards=(), held_as=jnp.bfloat16):
    values = scale * jax.random.normal(rng, shape, jnp.float32)
    if shards:
        values = values * level_of(rng, shape, shards, -0.22, 0.18)
    return jnp.clip(values, -limit, limit).astype(held_as)


def setup_inputs(seed: int = 0, part: int = 0) -> dict:
    arg_keys = jax.random.split(jax.random.key(seed), 11)
    own_keys = jax.random.split(jax.random.fold_in(arg_keys[10], part), 11)
    hidden = centred(own_keys[0], (NEW, MODEL_WIDTH), 1.0, 6.0)
    w_query = centred(arg_keys[1], (MODEL_WIDTH, QUERY_HEADS * HEAD_SIZE), MODEL_WIDTH ** -0.5, 0.078125, ((1, 64),))
    key_projection_weight = centred(arg_keys[2], (MODEL_WIDTH, KEY_VALUE_HEADS * HEAD_SIZE), MODEL_WIDTH ** -0.5, 0.078125, ((1, 64),))
    value_projection_weight = centred(arg_keys[3], (MODEL_WIDTH, KEY_VALUE_HEADS * HEAD_SIZE), MODEL_WIDTH ** -0.5, 0.078125, ((1, 64),))
    query_gain = jnp.clip(jnp.exp(jax.random.uniform(arg_keys[4], (HEAD_SIZE,), jnp.float32, math.log(0.5), math.log(1.5))), 0.5, 1.5)
    key_gain = jnp.clip(jnp.exp(jax.random.uniform(arg_keys[5], (HEAD_SIZE,), jnp.float32, math.log(4.0), math.log(8.0))), 4.0, 8.0)
    stored_cache_keys = draw_stored_cache_keys(jax.random.fold_in(jax.random.fold_in(arg_keys[10], part), 71), part)
    stored_cache_values = centred(own_keys[7], (CACHE_SLOTS, KEY_VALUE_HEADS * HEAD_SIZE), 2.0, 8.0, ((0, 64),))
    cache_length = jax.random.randint(own_keys[8], (1,), CACHE_SLOTS // 2, CACHE_SLOTS + 1).astype(jnp.int32)
    first_position = jax.random.randint(own_keys[9], (1,), 0, 4096).astype(jnp.int32)
    return dict(hidden=hidden, w_query=w_query, key_projection_weight=key_projection_weight, value_projection_weight=value_projection_weight, query_gain=query_gain, key_gain=key_gain, stored_cache_keys=stored_cache_keys, stored_cache_values=stored_cache_values, cache_length=cache_length, first_position=first_position)


def normalize(joined_values, gain):
    mean_square = lax.optimization_barrier(jnp.mean(joined_values * joined_values, axis=-1, keepdims=True))
    return joined_values * lax.rsqrt(mean_square + 1e-06) * gain

def rotate(joined_values, positions):
    half = joined_values.shape[-1] // 2
    freq = jnp.exp(jnp.arange(half, dtype=jnp.float32) * (-2.0 * math.log(1000000.0) / joined_values.shape[-1]))
    angles = positions[:, None] * freq[None, :]
    cosine = jnp.concatenate([jnp.cos(angles), jnp.cos(angles)], axis=-1)[:, None, :]
    sine = jnp.concatenate([jnp.sin(angles), jnp.sin(angles)], axis=-1)[:, None, :]
    turned = jnp.concatenate([-joined_values[..., half:], joined_values[..., :half]], axis=-1)
    return joined_values * cosine + turned * sine

def reference(hidden, w_query, key_projection_weight, value_projection_weight, query_gain, key_gain, stored_cache_keys, stored_cache_values, cache_length, first_position):
    input_tokens = hidden.shape[0]
    positions = first_position[0].astype(jnp.float32) + jnp.arange(input_tokens, dtype=jnp.float32)
    projected = jnp.dot(hidden, w_query, preferred_element_type=jnp.float32).reshape(input_tokens, QUERY_HEADS, HEAD_SIZE)
    query_states = rotate(normalize(projected, query_gain), positions).astype(jnp.bfloat16)
    key_unnormalized = jnp.dot(hidden, key_projection_weight, preferred_element_type=jnp.float32).astype(jnp.bfloat16)
    key_unnormalized = lax.optimization_barrier(key_unnormalized).astype(jnp.float32).reshape(input_tokens, HEAD_SIZE, KEY_VALUE_HEADS).transpose(0, 2, 1)
    incoming_keys = rotate(normalize(key_unnormalized, key_gain), positions).astype(jnp.bfloat16)
    incoming_values = jnp.dot(hidden, value_projection_weight, preferred_element_type=jnp.float32).astype(jnp.bfloat16).reshape(input_tokens, HEAD_SIZE, KEY_VALUE_HEADS).transpose(0, 2, 1)
    query_group = QUERY_HEADS // KEY_VALUE_HEADS
    token_rows = query_states.reshape(input_tokens, KEY_VALUE_HEADS, query_group, HEAD_SIZE).transpose(1, 2, 0, 3).reshape(KEY_VALUE_HEADS, query_group * input_tokens, HEAD_SIZE)
    joined_keys = jnp.concatenate([stored_cache_keys.reshape(CACHE_SLOTS, KEY_VALUE_HEADS, HEAD_SIZE).transpose(1, 0, 2), incoming_keys.transpose(1, 0, 2)], axis=1)
    joined_values = jnp.concatenate([stored_cache_values.reshape(CACHE_SLOTS, KEY_VALUE_HEADS, HEAD_SIZE).transpose(1, 0, 2), incoming_values.transpose(1, 0, 2)], axis=1)
    cached = jnp.arange(CACHE_SLOTS) < cache_length[0]
    token_of_row = jnp.arange(query_group * input_tokens) % input_tokens
    causal = jnp.arange(input_tokens)[None, :] <= token_of_row[:, None]
    visible = jnp.concatenate([jnp.broadcast_to(cached[None, :], (query_group * input_tokens, CACHE_SLOTS)), causal], axis=1)
    scale = 1.0 / math.sqrt(HEAD_SIZE)

    def one_head(operands):
        query_rows, key_rows, value_rows = operands
        scores = lax.dot_general(query_rows, key_rows, (((1,), (1,)), ((), ())), preferred_element_type=jnp.float32) * scale
        masked = jnp.where(visible, scores, -1e+30)
        top = lax.optimization_barrier(jnp.max(masked, axis=1, keepdims=True))
        weights = jnp.where(visible, jnp.exp(masked - top), 0.0)
        total = lax.optimization_barrier(jnp.sum(weights, axis=1, keepdims=True))
        mixed = jnp.dot(weights.astype(jnp.bfloat16), value_rows, preferred_element_type=jnp.float32)
        return mixed / total
    attention_output = lax.map(one_head, (token_rows, joined_keys, joined_values))
    attention_output = attention_output.reshape(KEY_VALUE_HEADS, query_group, input_tokens, HEAD_SIZE).transpose(2, 0, 1, 3).reshape(input_tokens, QUERY_HEADS * HEAD_SIZE)
    return attention_output.astype(jnp.bfloat16)
```

```python
import math

import jax
import jax.numpy as jnp
from jax import lax
from jax.experimental import pallas as pl
from jax.experimental.pallas import tpu as pltpu
from jax.sharding import Mesh
from jax.sharding import PartitionSpec as P

FAR = "far"
NEAR = ("near_z", "near_y", "core")
CTX = (FAR, *NEAR)
REQ_CTX = ("req", *CTX)

HIDDEN_MASK = -1e30
STAT_ROWS = 16


def normalize_columns(values, gain):
    mean_square = jnp.mean(values * values, axis=0, keepdims=True)
    return values * lax.rsqrt(mean_square + 1e-06) * gain[:, None]


def rotate_columns(values, cosine, sine):
    half = values.shape[0] // 2
    turned = jnp.concatenate([-values[half:], values[:half]], axis=0)
    return values * cosine + turned * sine


def angles_of(first_position, tokens, head_dim):
    half = head_dim // 2
    positions = first_position[0].astype(jnp.float32) + jnp.arange(tokens, dtype=jnp.float32)
    freq = jnp.exp(
        jnp.arange(half, dtype=jnp.float32) * (-2.0 * math.log(1000000.0) / head_dim)
    )
    angles = freq[:, None] * positions[None, :]
    cosine = jnp.cos(angles)
    sine = jnp.sin(angles)
    return (
        jnp.concatenate([cosine, cosine], axis=0),
        jnp.concatenate([sine, sine], axis=0),
    )


def shard_kernel(limit_ref, queries_ref, cache_ref, out_ref, values_ref, scores_ref):
    heads, head_dim, tokens = queries_ref.shape
    shards, _, slots, _ = cache_ref.shape
    scale = 1.0 / math.sqrt(head_dim)
    limit = limit_ref[0]
    near = limit_ref[1]
    for shard in range(shards):
        values_ref[:, shard * slots : (shard + 1) * slots] = cache_ref[shard, 1].T
    slot = lax.broadcasted_iota(jnp.int32, (slots, tokens), 0)

    def one_head(head, carry):
        query = queries_ref[head]
        top = jnp.full((1, tokens), HIDDEN_MASK, jnp.float32)
        for shard in range(shards):
            scores = (
                jnp.dot(cache_ref[shard, 0], query, preferred_element_type=jnp.float32) * scale
            )
            visible = slot < limit - (shard * 8 + near) * slots
            scores = jnp.where(visible, scores, HIDDEN_MASK)
            scores_ref[shard * slots : (shard + 1) * slots, :] = scores
            top = jnp.maximum(top, jnp.max(scores, axis=0, keepdims=True))
        top = top.astype(jnp.bfloat16).astype(jnp.float32)
        scores = scores_ref[...]
        weights = jnp.where(scores > 0.5 * HIDDEN_MASK, jnp.exp(scores - top), 0.0)
        total = jnp.sum(weights, axis=0, keepdims=True)
        summed = jnp.dot(
            values_ref[...], weights.astype(jnp.bfloat16), preferred_element_type=jnp.float32
        )
        high = total.astype(jnp.bfloat16).astype(jnp.float32)
        row = lax.broadcasted_iota(jnp.int32, (STAT_ROWS, tokens), 0)
        stats = jnp.where(row == 0, top, jnp.where(row == 1, high, total - high))
        out_ref[head, :head_dim, :] = summed.astype(jnp.bfloat16)
        out_ref[head, head_dim:, :] = stats.astype(jnp.bfloat16)
        return carry

    lax.fori_loop(0, heads, one_head, 0)


def final_kernel(query_ref, keys_ref, values_ref, received_ref, out_ref):
    head_dim, tokens = query_ref.shape
    sources = received_ref.shape[0]
    scale = 1.0 / math.sqrt(head_dim)
    scores = (
        lax.dot_general(
            keys_ref[...],
            query_ref[...],
            (((0,), (0,)), ((), ())),
            preferred_element_type=jnp.float32,
        )
        * scale
    )
    source = lax.broadcasted_iota(jnp.int32, (tokens, tokens), 0)
    token = lax.broadcasted_iota(jnp.int32, (tokens, tokens), 1)
    causal = source <= token
    scores = jnp.where(causal, scores, HIDDEN_MASK)
    top = jnp.max(scores, axis=0, keepdims=True)
    stats = [
        received_ref[k, head_dim : head_dim + STAT_ROWS, :].astype(jnp.float32)
        for k in range(sources)
    ]
    for k in range(sources):
        top = jnp.maximum(top, stats[k][0:1])
    weights = jnp.where(causal, jnp.exp(scores - top), 0.0)
    total = jnp.sum(weights, axis=0, keepdims=True)
    summed = jnp.dot(
        values_ref[...], weights.astype(jnp.bfloat16), preferred_element_type=jnp.float32
    )
    for k in range(sources):
        factor = jnp.exp(stats[k][0:1] - top)
        total = total + factor * (stats[k][1:2] + stats[k][2:3])
        summed = summed + factor * received_ref[k, :head_dim, :].astype(jnp.float32)
    out_ref[...] = (summed / total).T.astype(jnp.bfloat16)


def per_device(
    hidden,
    w_query,
    key_projection_weight,
    value_projection_weight,
    query_gain,
    key_gain,
    stored_cache_keys,
    stored_cache_values,
    cache_length,
    first_position,
):
    tokens = hidden.shape[0]
    head_dim = query_gain.shape[0]
    slots = stored_cache_keys.shape[0]
    kv_heads = stored_cache_keys.shape[1] // head_dim
    near = lax.axis_index(NEAR)
    near_size = lax.axis_size(NEAR)
    far_size = lax.axis_size(FAR)

    cache = jnp.stack(
        [
            stored_cache_keys.reshape(slots, kv_heads, head_dim).transpose(1, 0, 2),
            stored_cache_values.reshape(slots, kv_heads, head_dim).transpose(1, 0, 2),
        ],
        axis=1,
    )
    cache = lax.all_to_all(cache, FAR, 0, 0, tiled=True)

    weights = (((0,), (1,)), ((), ()))
    key_part = lax.dot_general(
        key_projection_weight, hidden, weights, preferred_element_type=jnp.float32
    ).astype(jnp.bfloat16)
    value_part = lax.dot_general(
        value_projection_weight, hidden, weights, preferred_element_type=jnp.float32
    ).astype(jnp.bfloat16)
    part = jnp.stack([key_part, value_part]).reshape(2, -1, kv_heads, tokens)
    entries = part.shape[1]
    part = part.transpose(2, 0, 1, 3).reshape(kv_heads, 2 * entries, tokens)
    part = lax.all_to_all(part, FAR, 0, 0, tiled=True)

    cosine, sine = angles_of(first_position, tokens, head_dim)
    projected = lax.dot_general(w_query, hidden, weights, preferred_element_type=jnp.float32)
    own_query = rotate_columns(normalize_columns(projected, query_gain), cosine, sine).astype(
        jnp.bfloat16
    )
    both = jnp.concatenate([own_query, part.reshape(-1, tokens)], axis=0)
    gathered = lax.all_gather(both, NEAR)
    queries = gathered[:, :head_dim]
    fresh = gathered[:, head_dim:].reshape(near_size, far_size, 2, entries, tokens)
    fresh = fresh.transpose(2, 1, 0, 3, 4).reshape(2, head_dim, tokens)
    new_keys = rotate_columns(
        normalize_columns(fresh[0].astype(jnp.float32), key_gain), cosine, sine
    ).astype(jnp.bfloat16)
    new_values = fresh[1]

    limits = jnp.stack([cache_length[0], near.astype(jnp.int32)])
    partial = pl.pallas_call(
        shard_kernel,
        out_shape=jax.ShapeDtypeStruct(
            (near_size, head_dim + STAT_ROWS, tokens), jnp.bfloat16
        ),
        in_specs=[
            pl.BlockSpec(memory_space=pltpu.SMEM),
            pl.BlockSpec(memory_space=pltpu.VMEM),
            pl.BlockSpec(memory_space=pltpu.VMEM),
        ],
        out_specs=pl.BlockSpec(memory_space=pltpu.VMEM),
        scratch_shapes=[
            pltpu.VMEM((head_dim, far_size * slots), jnp.bfloat16),
            pltpu.VMEM((far_size * slots, tokens), jnp.float32),
        ],
        cost_estimate=pl.CostEstimate(
            flops=4 * near_size * tokens * head_dim * far_size * slots,
            bytes_accessed=1 << 20,
            transcendentals=near_size * tokens * far_size * slots,
        ),
        name="cache_term",
    )(limits, queries, cache)
    received = lax.all_to_all(partial, NEAR, 0, 0, tiled=True)
    return pl.pallas_call(
        final_kernel,
        out_shape=jax.ShapeDtypeStruct((tokens, head_dim), jnp.bfloat16),
        name="final_join",
    )(own_query, new_keys, new_values, received)


def solution(mesh):
    finer = Mesh(
        mesh.devices.reshape(8, 2, 2, 2, mesh.shape["req"]),
        (*CTX, "req"),
    )
    return jax.shard_map(
        per_device,
        mesh=finer,
        in_specs=(
            P("req", None),
            P(None, CTX),
            P(None, CTX),
            P(None, CTX),
            P(),
            P(),
            P(REQ_CTX, None),
            P(REQ_CTX, None),
            P("req"),
            P("req"),
        ),
        out_specs=P("req", CTX),
        check_vma=False,
    )
```

```python
import math

import jax
import jax.numpy as jnp
from jax import lax
from jax.experimental import pallas as pl
from jax.experimental.pallas import tpu as pltpu
from jax.sharding import PartitionSpec as P

FARS = 8
LOWS = 4
LINE = 2 * LOWS
NEVER = -1e30
FLOOR = -1e29
PART_ROWS = 8
STAT_ROWS = 8


def side_of(lane, far):
    return lane ^ 1 if far < FARS // 2 else lane


def rank_of(far, lane, low):
    return far * LINE + side_of(lane, far) * LOWS + low


LINES = [
    [rank_of(far, lane, low) for far in range(FARS)] for lane in range(2) for low in range(LOWS)
]
NEARS = [
    [rank_of(far, lane, low) for lane in range(2) for low in range(LOWS)] for far in range(FARS)
]
CORE_PAIRS = [[r, r + 1] for r in range(FARS * LINE) if r % 2 == 0]
ROW_PAIRS = [[r, r + 2] for r in range(FARS * LINE) if r // 2 % 2 == 0]
LANE_PAIRS = [
    [rank_of(far, lane, low) for lane in range(2)] for far in range(FARS) for low in range(LOWS)
]

WHOLE = pltpu.CompilerParams(vmem_limit_bytes=67043328)
SMALL = pltpu.CompilerParams(vmem_limit_bytes=24 << 20)
VMEM = pl.BlockSpec(memory_space=pltpu.VMEM)
HBM = pl.BlockSpec(memory_space=pltpu.HBM)
SMEM = pl.BlockSpec(memory_space=pltpu.SMEM)


def pack_kernel(
    hidden_hbm,
    key_weight_hbm,
    value_weight_hbm,
    keys_hbm,
    values_hbm,
    out_hbm,
    hidden_ref,
    key_weight_ref,
    value_weight_ref,
    keys_ref,
    values_ref,
    part_ref,
    in_sems,
    key_sems,
    value_sems,
    part_sems,
):
    slots = keys_ref.shape[0]
    head_dim = keys_ref.shape[1] // FARS
    loads = [
        pltpu.make_async_copy(source, target, in_sems.at[k])
        for k, (source, target) in enumerate(
            (
                (keys_hbm, keys_ref),
                (values_hbm, values_ref),
                (hidden_hbm, hidden_ref),
                (key_weight_hbm, key_weight_ref),
                (value_weight_hbm, value_weight_ref),
            )
        )
    ]
    for load in loads:
        load.start()
    stores = []
    for k, (ref, sems) in enumerate(((keys_ref, key_sems), (values_ref, value_sems))):
        loads[k].wait()
        for far in range(FARS):
            store = pltpu.make_async_copy(
                ref.at[:, pl.ds(far * head_dim, head_dim)],
                out_hbm.at[far, pl.ds(k * slots, slots), :],
                sems.at[far],
            )
            store.start()
            stores.append(store)
    for load in loads[2:]:
        load.wait()
    across = (((1,), (1,)), ((), ()))
    key_part, value_part = [
        lax.dot_general(ref[...], hidden_ref[...], across, preferred_element_type=jnp.float32)
        for ref in (key_weight_ref, value_weight_ref)
    ]
    entries = key_part.shape[0] // FARS
    rows = jnp.concatenate([key_part, value_part], axis=0)
    target = lax.broadcasted_iota(jnp.int32, (FARS * PART_ROWS, rows.shape[0]), 0)
    source = lax.broadcasted_iota(jnp.int32, (FARS * PART_ROWS, rows.shape[0]), 1)
    inside = target % PART_ROWS
    pick = (inside < 2 * entries) & (source == inside * FARS + target // PART_ROWS)
    ordered = jnp.dot(
        pick.astype(jnp.bfloat16), rows.astype(jnp.bfloat16), preferred_element_type=jnp.float32
    ).astype(jnp.bfloat16)
    for far in range(FARS):
        part_ref[far] = ordered[far * PART_ROWS : (far + 1) * PART_ROWS]
        store = pltpu.make_async_copy(
            part_ref.at[far], out_hbm.at[far, pl.ds(2 * slots, PART_ROWS), :], part_sems.at[far]
        )
        store.start()
        stores.append(store)
    for store in stores:
        store.wait()


def cache_kernel(limit_ref, queries_ref, cache_ref, out_ref, turned_ref, scores_ref, weights_ref):
    heads, head_dim, tokens = queries_ref.shape
    slots = (cache_ref.shape[1] - PART_ROWS) // 2
    factor = math.log2(math.e) / math.sqrt(head_dim)
    pairs = heads // 2
    wide = 2 * tokens
    for far in range(FARS):
        turned_ref[:, far * slots : (far + 1) * slots] = cache_ref[far, slots : 2 * slots].T
    slot = lax.broadcasted_iota(jnp.int32, (slots, wide), 0)

    rows = jnp.concatenate([cache_ref[far, 2 * slots :] for far in range(FARS)], axis=0)
    entries = head_dim // (FARS * LINE)
    kept = 2 * entries * FARS
    target = lax.broadcasted_iota(jnp.int32, (kept, FARS * PART_ROWS), 0)
    source = lax.broadcasted_iota(jnp.int32, (kept, FARS * PART_ROWS), 1)
    kind, place = target // (entries * FARS), target % (entries * FARS)
    wanted = (place // entries) * PART_ROWS + kind * entries + place % entries
    part = jnp.dot(
        (source == wanted).astype(jnp.bfloat16), rows, preferred_element_type=jnp.float32
    ).astype(jnp.bfloat16)
    for head in range(heads):
        out_ref[head, head_dim : head_dim + kept, :] = part

    def score(pair):
        query = jnp.concatenate([queries_ref[2 * pair], queries_ref[2 * pair + 1]], axis=1)
        top = jnp.full((1, wide), FLOOR, jnp.float32)
        for far in range(FARS):
            scores = jnp.dot(cache_ref[far, :slots], query, preferred_element_type=jnp.float32)
            scores = jnp.where(slot < limit_ref[far], scores, NEVER)
            scores_ref[pair, far * slots : (far + 1) * slots, :] = scores
            top = jnp.maximum(top, jnp.max(scores, axis=0, keepdims=True))
        return top.astype(jnp.bfloat16).astype(jnp.float32)

    def mix(pair, top):
        total = jnp.zeros((1, wide), jnp.float32)
        for far in range(FARS):
            block = slice(far * slots, (far + 1) * slots)
            weights = jnp.exp2((scores_ref[pair, block, :] - top) * factor)
            total = total + jnp.sum(weights, axis=0, keepdims=True)
            weights_ref[pair, block, :] = weights.astype(jnp.bfloat16)
        summed = jnp.dot(turned_ref[...], weights_ref[pair], preferred_element_type=jnp.float32)
        high = total.astype(jnp.bfloat16).astype(jnp.float32)
        row = lax.broadcasted_iota(jnp.int32, (STAT_ROWS, wide), 0)
        stats = jnp.where(row == 0, top, jnp.where(row == 1, high, total - high))
        for half in range(2):
            columns = slice(half * tokens, (half + 1) * tokens)
            out_ref[2 * pair + half, :head_dim, :] = summed[:, columns].astype(jnp.bfloat16)
            out_ref[2 * pair + half, head_dim + kept :, :] = stats[:, columns].astype(jnp.bfloat16)

    top = score(0)
    for pair in range(pairs):
        following = score(pair + 1) if pair + 1 < pairs else None
        mix(pair, top)
        top = following


def final_kernel(query_ref, received_ref, gain_ref, cosine_ref, sine_ref, out_ref):
    head_dim, tokens = query_ref.shape
    factor = math.log2(math.e) / math.sqrt(head_dim)
    entries = head_dim // (FARS * LINE)
    span = entries * FARS
    entry = lax.broadcasted_iota(jnp.int32, (head_dim, head_dim), 0)
    place = lax.broadcasted_iota(jnp.int32, (head_dim, head_dim), 1)
    lane, low = place // (span * LOWS), place // span % LOWS
    far = place % span // entries
    side = jnp.where(far < FARS // 2, 1 - lane, lane)
    wanted = ((far * 2 + side) * LOWS + low) * entries + place % entries
    pick = (entry == wanted).astype(jnp.bfloat16)

    def gathered(kind):
        first = head_dim + kind * span
        rows = jnp.concatenate([received_ref[k, first : first + span] for k in range(LINE)], axis=0)
        return jnp.dot(pick, rows, preferred_element_type=jnp.float32)

    raw = gathered(0)
    mean_square = jnp.mean(raw * raw, axis=0, keepdims=True)
    normed = raw * lax.rsqrt(mean_square + 1e-06) * gain_ref[...]
    half = head_dim // 2
    turned = jnp.concatenate([-normed[half:], normed[:half]], axis=0)
    new_keys = (normed * cosine_ref[...] + turned * sine_ref[...]).astype(jnp.bfloat16)
    new_values = gathered(1).astype(jnp.bfloat16)
    scores = jnp.dot(new_keys.T, query_ref[...], preferred_element_type=jnp.float32)
    source = lax.broadcasted_iota(jnp.int32, (tokens, tokens), 0)
    token = lax.broadcasted_iota(jnp.int32, (tokens, tokens), 1)
    scores = jnp.where(source <= token, scores, NEVER)
    top = jnp.max(scores, axis=0, keepdims=True)
    first = head_dim + 2 * span
    stats = [received_ref[k, first : first + STAT_ROWS].astype(jnp.float32) for k in range(LINE)]
    for k in range(LINE):
        top = jnp.maximum(top, stats[k][0:1])
    weights = jnp.exp2((scores - top) * factor)
    total = jnp.sum(weights, axis=0, keepdims=True)
    summed = jnp.dot(new_values, weights.astype(jnp.bfloat16), preferred_element_type=jnp.float32)
    for k in range(LINE):
        share = jnp.exp2((stats[k][0:1] - top) * factor)
        total = total + share * (stats[k][1:2] + stats[k][2:3])
        summed = summed + share * received_ref[k, :head_dim].astype(jnp.float32)
    out_ref[...] = (summed / total).T.astype(jnp.bfloat16)


def angles_of(first_position, tokens, head_dim):
    half = head_dim // 2
    positions = first_position[0].astype(jnp.float32) + jnp.arange(tokens, dtype=jnp.float32)
    freq = jnp.exp(jnp.arange(half, dtype=jnp.float32) * (-2.0 * math.log(1000000.0) / head_dim))
    angles = freq[:, None] * positions[None, :]
    cosine, sine = jnp.cos(angles), jnp.sin(angles)
    return jnp.concatenate([cosine, cosine], axis=0), jnp.concatenate([sine, sine], axis=0)


def query_kernel(hidden_ref, weight_ref, gain_ref, cosine_ref, sine_ref, own_ref):
    projected = jnp.dot(hidden_ref[...], weight_ref[...], preferred_element_type=jnp.float32)
    mean_square = jnp.mean(projected * projected, axis=1, keepdims=True)
    normed = (projected * lax.rsqrt(mean_square + 1e-06) * gain_ref[...]).T
    half = normed.shape[0] // 2
    turned = jnp.concatenate([-normed[half:], normed[:half]], axis=0)
    own_ref[...] = (normed * cosine_ref[...] + turned * sine_ref[...]).astype(jnp.bfloat16)


def per_device(
    hidden,
    w_query,
    key_projection_weight,
    value_projection_weight,
    query_gain,
    key_gain,
    stored_cache_keys,
    stored_cache_values,
    cache_length,
    first_position,
):
    tokens = hidden.shape[0]
    head_dim = query_gain.shape[0]
    slots = stored_cache_keys.shape[0]
    entries = key_projection_weight.shape[1] // FARS
    rank = lax.axis_index("ctx")

    packed = pl.pallas_call(
        pack_kernel,
        out_shape=jax.ShapeDtypeStruct((FARS, 2 * slots + PART_ROWS, head_dim), jnp.bfloat16),
        in_specs=[HBM] * 5,
        out_specs=HBM,
        scratch_shapes=[
            pltpu.VMEM(hidden.shape, jnp.bfloat16),
            pltpu.VMEM(key_projection_weight.shape[::-1], jnp.bfloat16),
            pltpu.VMEM(value_projection_weight.shape[::-1], jnp.bfloat16),
            pltpu.VMEM(stored_cache_keys.shape, jnp.bfloat16),
            pltpu.VMEM(stored_cache_values.shape, jnp.bfloat16),
            pltpu.VMEM((FARS, PART_ROWS, tokens), jnp.bfloat16),
            pltpu.SemaphoreType.DMA((5,)),
            pltpu.SemaphoreType.DMA((FARS,)),
            pltpu.SemaphoreType.DMA((FARS,)),
            pltpu.SemaphoreType.DMA((FARS,)),
        ],
        compiler_params=WHOLE,
        cost_estimate=pl.CostEstimate(flops=1 << 26, bytes_accessed=1 << 22, transcendentals=0),
        name="pack",
    )(
        hidden,
        key_projection_weight.T,
        value_projection_weight.T,
        stored_cache_keys,
        stored_cache_values,
    )
    cache = lax.all_to_all(packed, "ctx", 0, 0, axis_index_groups=LINES, tiled=True)

    cosine, sine = angles_of(first_position, tokens, head_dim)
    own_query = pl.pallas_call(
        query_kernel,
        out_shape=jax.ShapeDtypeStruct((head_dim, tokens), jnp.bfloat16),
        in_specs=[VMEM] * 5,
        out_specs=VMEM,
        compiler_params=SMALL,
        cost_estimate=pl.CostEstimate(flops=1 << 28, bytes_accessed=1 << 21, transcendentals=0),
        name="query",
    )(hidden, w_query, query_gain[None], cosine, sine)
    queries = own_query[None]
    for pairs in (CORE_PAIRS, ROW_PAIRS, LANE_PAIRS):
        queries = lax.all_gather(queries, "ctx", axis_index_groups=pairs, tiled=True)

    far = jnp.arange(FARS, dtype=jnp.int32)
    turned = (far < FARS // 2).astype(jnp.int32)
    own_turned = (rank < FARS // 2 * LINE).astype(jnp.int32)
    lane = (rank // LOWS % 2) ^ own_turned
    shard = far * LINE + (lane ^ turned) * LOWS + rank % LOWS
    limits = cache_length[0] - shard * slots

    kept = 2 * entries * FARS
    partial = pl.pallas_call(
        cache_kernel,
        out_shape=jax.ShapeDtypeStruct((LINE, head_dim + kept + STAT_ROWS, tokens), jnp.bfloat16),
        in_specs=[SMEM, VMEM, VMEM],
        out_specs=VMEM,
        scratch_shapes=[
            pltpu.VMEM((head_dim, FARS * slots), jnp.bfloat16),
            pltpu.VMEM((LINE // 2, FARS * slots, 2 * tokens), jnp.float32),
            pltpu.VMEM((LINE // 2, FARS * slots, 2 * tokens), jnp.bfloat16),
        ],
        compiler_params=SMALL,
        cost_estimate=pl.CostEstimate(
            flops=4 * LINE * tokens * head_dim * FARS * slots,
            bytes_accessed=1 << 20,
            transcendentals=LINE * tokens * FARS * slots,
        ),
        name="cache_term",
    )(limits, queries, cache)
    received = lax.all_to_all(partial, "ctx", 0, 0, axis_index_groups=NEARS, tiled=True)
    gain = jnp.broadcast_to(key_gain[:, None], (head_dim, tokens))
    return pl.pallas_call(
        final_kernel,
        out_shape=jax.ShapeDtypeStruct((tokens, head_dim), jnp.bfloat16),
        in_specs=[VMEM] * 5,
        out_specs=VMEM,
        compiler_params=SMALL,
        name="final_join",
    )(own_query, received, gain, cosine, sine)


def solution(mesh):
    return jax.shard_map(
        per_device,
        mesh=mesh,
        in_specs=(
            P("req", None),
            P(None, "ctx"),
            P(None, "ctx"),
            P(None, "ctx"),
            P(),
            P(),
            P(("req", "ctx"), None),
            P(("req", "ctx"), None),
            P("req"),
            P("req"),
        ),
        out_specs=P("req", "ctx"),
        check_vma=False,
    )
```

```python
import math

import jax
import jax.numpy as jnp
from jax import lax
from jax.experimental import pallas as pl
from jax.experimental.pallas import tpu as pltpu
from jax.sharding import PartitionSpec as P

FARS = 8
LOWS = 4
LINE = 2 * LOWS
NEVER = -1e30
FLOOR = -1e29
PART_ROWS = 8
STAT_ROWS = 8
HIDDEN_CHUNKS = 4


def side_of(lane, far):
    return lane ^ 1 if far < FARS // 2 else lane


def rank_of(far, lane, low):
    return far * LINE + side_of(lane, far) * LOWS + low


ORDER = (0, 4, 1, 5, 2, 6, 3, 7)
LINES = [[rank_of(far, lane, low) for far in ORDER] for lane in range(2) for low in range(LOWS)]
NEARS = [
    [rank_of(far, lane, low) for lane in range(2) for low in range(LOWS)] for far in range(FARS)
]
CORE_PAIRS = [[r, r + 1] for r in range(FARS * LINE) if r % 2 == 0]
ROW_PAIRS = [[r, r + 2] for r in range(FARS * LINE) if r // 2 % 2 == 0]
LANE_PAIRS = [
    [rank_of(far, lane, low) for lane in range(2)] for far in range(FARS) for low in range(LOWS)
]

WHOLE = pltpu.CompilerParams(vmem_limit_bytes=67043328)
SMALL = pltpu.CompilerParams(vmem_limit_bytes=24 << 20)
VMEM = pl.BlockSpec(memory_space=pltpu.VMEM)
HBM = pl.BlockSpec(memory_space=pltpu.HBM)
SMEM = pl.BlockSpec(memory_space=pltpu.SMEM)


def pack_kernel(
    hidden_hbm,
    key_weight_hbm,
    value_weight_hbm,
    keys_hbm,
    values_hbm,
    out_hbm,
    hidden_ref,
    weight_ref,
    cache_ref,
    part_ref,
    hidden_sems,
    weight_sems,
    cache_sems,
    store_sems,
    part_sems,
):
    slots = keys_hbm.shape[0]
    head_dim = keys_hbm.shape[1] // FARS
    columns = key_weight_hbm.shape[0]
    depth = hidden_hbm.shape[1] // HIDDEN_CHUNKS
    cache_loads = [
        pltpu.make_async_copy(source, cache_ref.at[k], cache_sems.at[k])
        for k, source in enumerate((keys_hbm, values_hbm))
    ]
    weight_loads = [
        pltpu.make_async_copy(
            source, weight_ref.at[pl.ds(k * columns, columns), :], weight_sems.at[k]
        )
        for k, source in enumerate((key_weight_hbm, value_weight_hbm))
    ]
    hidden_loads = [
        pltpu.make_async_copy(
            hidden_hbm.at[:, pl.ds(k * depth, depth)],
            hidden_ref.at[:, pl.ds(k * depth, depth)],
            hidden_sems.at[k],
        )
        for k in range(HIDDEN_CHUNKS)
    ]
    for load in weight_loads + hidden_loads[:2] + cache_loads + hidden_loads[2:]:
        load.start()
    entries = columns // FARS
    shape = (FARS * PART_ROWS, 2 * columns)
    target = lax.broadcasted_iota(jnp.int32, shape, 0)
    source = lax.broadcasted_iota(jnp.int32, shape, 1)
    inside = target % PART_ROWS
    pick = (inside < 2 * entries) & (source == inside * FARS + target // PART_ROWS)
    pick = pick.astype(jnp.bfloat16)
    for load in weight_loads:
        load.wait()
    across = (((1,), (1,)), ((), ()))
    stores = []
    total = None
    for k in range(HIDDEN_CHUNKS):
        hidden_loads[k].wait()
        block = slice(k * depth, (k + 1) * depth)
        term = lax.dot_general(
            hidden_ref[:, block], weight_ref[:, block], across, preferred_element_type=jnp.float32
        )
        total = term if total is None else total + term
        if k == 1:
            for kind, load in enumerate(cache_loads):
                load.wait()
                for far in range(FARS):
                    store = pltpu.make_async_copy(
                        cache_ref.at[kind, :, pl.ds(far * head_dim, head_dim)],
                        out_hbm.at[ORDER.index(far), pl.ds(kind * slots, slots), :],
                        store_sems.at[kind, far],
                    )
                    store.start()
                    stores.append(store)
    ordered = jnp.dot(
        pick, total.T.astype(jnp.bfloat16), preferred_element_type=jnp.float32
    ).astype(jnp.bfloat16)
    for far in range(FARS):
        part_ref[far] = ordered[far * PART_ROWS : (far + 1) * PART_ROWS]
        store = pltpu.make_async_copy(
            part_ref.at[far],
            out_hbm.at[ORDER.index(far), pl.ds(2 * slots, PART_ROWS), :],
            part_sems.at[far],
        )
        store.start()
        stores.append(store)
    for store in stores:
        store.wait()


def cache_kernel(limit_ref, queries_ref, cache_ref, out_ref, turned_ref, scores_ref, weights_ref):
    heads, head_dim, tokens = queries_ref.shape
    slots = (cache_ref.shape[1] - PART_ROWS) // 2
    factor = math.log2(math.e) / math.sqrt(head_dim)
    pairs = heads // 2
    wide = 2 * tokens
    for far in range(FARS):
        turned_ref[:, far * slots : (far + 1) * slots] = cache_ref[far, slots : 2 * slots].T
    slot = lax.broadcasted_iota(jnp.int32, (slots, wide), 0)

    rows = jnp.concatenate(
        [cache_ref[ORDER.index(far), 2 * slots :] for far in range(FARS)], axis=0
    )
    entries = head_dim // (FARS * LINE)
    kept = 2 * entries * FARS
    target = lax.broadcasted_iota(jnp.int32, (kept, FARS * PART_ROWS), 0)
    source = lax.broadcasted_iota(jnp.int32, (kept, FARS * PART_ROWS), 1)
    kind, place = target // (entries * FARS), target % (entries * FARS)
    wanted = (place // entries) * PART_ROWS + kind * entries + place % entries
    part = jnp.dot(
        (source == wanted).astype(jnp.bfloat16), rows, preferred_element_type=jnp.float32
    ).astype(jnp.bfloat16)
    for head in range(heads):
        out_ref[head, head_dim : head_dim + kept, :] = part

    def score(pair):
        query = jnp.concatenate([queries_ref[2 * pair], queries_ref[2 * pair + 1]], axis=1)
        top = jnp.full((1, wide), FLOOR, jnp.float32)
        for far in range(FARS):
            scores = jnp.dot(cache_ref[far, :slots], query, preferred_element_type=jnp.float32)
            scores = jnp.where(slot < limit_ref[far], scores, NEVER)
            scores_ref[pair, far * slots : (far + 1) * slots, :] = scores
            top = jnp.maximum(top, jnp.max(scores, axis=0, keepdims=True))
        return top.astype(jnp.bfloat16).astype(jnp.float32)

    def mix(pair, top):
        total = jnp.zeros((1, wide), jnp.float32)
        for far in range(FARS):
            block = slice(far * slots, (far + 1) * slots)
            weights = jnp.exp2((scores_ref[pair, block, :] - top) * factor)
            total = total + jnp.sum(weights, axis=0, keepdims=True)
            weights_ref[pair, block, :] = weights.astype(jnp.bfloat16)
        summed = jnp.dot(turned_ref[...], weights_ref[pair], preferred_element_type=jnp.float32)
        high = total.astype(jnp.bfloat16).astype(jnp.float32)
        row = lax.broadcasted_iota(jnp.int32, (STAT_ROWS, wide), 0)
        stats = jnp.where(row == 0, top, jnp.where(row == 1, high, total - high))
        for half in range(2):
            columns = slice(half * tokens, (half + 1) * tokens)
            out_ref[2 * pair + half, :head_dim, :] = summed[:, columns].astype(jnp.bfloat16)
            out_ref[2 * pair + half, head_dim + kept :, :] = stats[:, columns].astype(jnp.bfloat16)

    top = score(0)
    for pair in range(pairs):
        following = score(pair + 1) if pair + 1 < pairs else None
        mix(pair, top)
        top = following


def final_kernel(query_ref, received_ref, gain_ref, cosine_ref, sine_ref, out_ref):
    head_dim, tokens = query_ref.shape
    factor = math.log2(math.e) / math.sqrt(head_dim)
    entries = head_dim // (FARS * LINE)
    span = entries * FARS
    entry = lax.broadcasted_iota(jnp.int32, (head_dim, head_dim), 0)
    place = lax.broadcasted_iota(jnp.int32, (head_dim, head_dim), 1)
    lane, low = place // (span * LOWS), place // span % LOWS
    far = place % span // entries
    side = jnp.where(far < FARS // 2, 1 - lane, lane)
    wanted = ((far * 2 + side) * LOWS + low) * entries + place % entries
    pick = (entry == wanted).astype(jnp.bfloat16)

    def gathered(kind):
        first = head_dim + kind * span
        rows = jnp.concatenate([received_ref[k, first : first + span] for k in range(LINE)], axis=0)
        return jnp.dot(pick, rows, preferred_element_type=jnp.float32)

    raw = gathered(0)
    mean_square = jnp.mean(raw * raw, axis=0, keepdims=True)
    normed = raw * lax.rsqrt(mean_square + 1e-06) * gain_ref[...]
    half = head_dim // 2
    turned = jnp.concatenate([-normed[half:], normed[:half]], axis=0)
    new_keys = (normed * cosine_ref[...] + turned * sine_ref[...]).astype(jnp.bfloat16)
    new_values = gathered(1).astype(jnp.bfloat16)
    scores = jnp.dot(new_keys.T, query_ref[...], preferred_element_type=jnp.float32)
    source = lax.broadcasted_iota(jnp.int32, (tokens, tokens), 0)
    token = lax.broadcasted_iota(jnp.int32, (tokens, tokens), 1)
    scores = jnp.where(source <= token, scores, NEVER)
    top = jnp.max(scores, axis=0, keepdims=True)
    first = head_dim + 2 * span
    stats = [received_ref[k, first : first + STAT_ROWS].astype(jnp.float32) for k in range(LINE)]
    for k in range(LINE):
        top = jnp.maximum(top, stats[k][0:1])
    weights = jnp.exp2((scores - top) * factor)
    total = jnp.sum(weights, axis=0, keepdims=True)
    summed = jnp.dot(new_values, weights.astype(jnp.bfloat16), preferred_element_type=jnp.float32)
    for k in range(LINE):
        share = jnp.exp2((stats[k][0:1] - top) * factor)
        total = total + share * (stats[k][1:2] + stats[k][2:3])
        summed = summed + share * received_ref[k, :head_dim].astype(jnp.float32)
    out_ref[...] = (summed / total).T.astype(jnp.bfloat16)


def angles_of(first_position, tokens, head_dim):
    half = head_dim // 2
    positions = first_position[0].astype(jnp.float32) + jnp.arange(tokens, dtype=jnp.float32)
    freq = jnp.exp(jnp.arange(half, dtype=jnp.float32) * (-2.0 * math.log(1000000.0) / head_dim))
    angles = freq[:, None] * positions[None, :]
    cosine, sine = jnp.cos(angles), jnp.sin(angles)
    return jnp.concatenate([cosine, cosine], axis=0), jnp.concatenate([sine, sine], axis=0)


def query_kernel(hidden_ref, weight_ref, gain_ref, cosine_ref, sine_ref, own_ref):
    projected = jnp.dot(hidden_ref[...], weight_ref[...], preferred_element_type=jnp.float32)
    mean_square = jnp.mean(projected * projected, axis=1, keepdims=True)
    normed = (projected * lax.rsqrt(mean_square + 1e-06) * gain_ref[...]).T
    half = normed.shape[0] // 2
    turned = jnp.concatenate([-normed[half:], normed[:half]], axis=0)
    own_ref[...] = (normed * cosine_ref[...] + turned * sine_ref[...]).astype(jnp.bfloat16)


def per_device(
    hidden,
    w_query,
    key_projection_weight,
    value_projection_weight,
    query_gain,
    key_gain,
    stored_cache_keys,
    stored_cache_values,
    cache_length,
    first_position,
):
    tokens = hidden.shape[0]
    head_dim = query_gain.shape[0]
    slots = stored_cache_keys.shape[0]
    entries = key_projection_weight.shape[1] // FARS
    rank = lax.axis_index("ctx")

    packed = pl.pallas_call(
        pack_kernel,
        out_shape=jax.ShapeDtypeStruct((FARS, 2 * slots + PART_ROWS, head_dim), jnp.bfloat16),
        in_specs=[HBM] * 5,
        out_specs=HBM,
        scratch_shapes=[
            pltpu.VMEM(hidden.shape, jnp.bfloat16),
            pltpu.VMEM((2 * key_projection_weight.shape[1], hidden.shape[1]), jnp.bfloat16),
            pltpu.VMEM((2, *stored_cache_keys.shape), jnp.bfloat16),
            pltpu.VMEM((FARS, PART_ROWS, tokens), jnp.bfloat16),
            pltpu.SemaphoreType.DMA((HIDDEN_CHUNKS,)),
            pltpu.SemaphoreType.DMA((2,)),
            pltpu.SemaphoreType.DMA((2,)),
            pltpu.SemaphoreType.DMA((2, FARS)),
            pltpu.SemaphoreType.DMA((FARS,)),
        ],
        compiler_params=WHOLE,
        cost_estimate=pl.CostEstimate(flops=1 << 26, bytes_accessed=1 << 22, transcendentals=0),
        name="pack",
    )(
        hidden,
        key_projection_weight.T,
        value_projection_weight.T,
        stored_cache_keys,
        stored_cache_values,
    )
    cache = lax.all_to_all(packed, "ctx", 0, 0, axis_index_groups=LINES, tiled=True)

    cosine, sine = angles_of(first_position, tokens, head_dim)
    own_query = pl.pallas_call(
        query_kernel,
        out_shape=jax.ShapeDtypeStruct((head_dim, tokens), jnp.bfloat16),
        in_specs=[VMEM] * 5,
        out_specs=VMEM,
        compiler_params=SMALL,
        cost_estimate=pl.CostEstimate(flops=1 << 28, bytes_accessed=1 << 21, transcendentals=0),
        name="query",
    )(hidden, w_query, query_gain[None], cosine, sine)
    queries = own_query[None]
    for pairs in (CORE_PAIRS, ROW_PAIRS, LANE_PAIRS):
        queries = lax.all_gather(queries, "ctx", axis_index_groups=pairs, tiled=True)

    far = jnp.array(ORDER, jnp.int32)
    turned = (far < FARS // 2).astype(jnp.int32)
    own_turned = (rank < FARS // 2 * LINE).astype(jnp.int32)
    lane = (rank // LOWS % 2) ^ own_turned
    shard = far * LINE + (lane ^ turned) * LOWS + rank % LOWS
    limits = cache_length[0] - shard * slots

    kept = 2 * entries * FARS
    partial = pl.pallas_call(
        cache_kernel,
        out_shape=jax.ShapeDtypeStruct((LINE, head_dim + kept + STAT_ROWS, tokens), jnp.bfloat16),
        in_specs=[SMEM, VMEM, VMEM],
        out_specs=VMEM,
        scratch_shapes=[
            pltpu.VMEM((head_dim, FARS * slots), jnp.bfloat16),
            pltpu.VMEM((LINE // 2, FARS * slots, 2 * tokens), jnp.float32),
            pltpu.VMEM((LINE // 2, FARS * slots, 2 * tokens), jnp.bfloat16),
        ],
        compiler_params=SMALL,
        cost_estimate=pl.CostEstimate(
            flops=4 * LINE * tokens * head_dim * FARS * slots,
            bytes_accessed=1 << 20,
            transcendentals=LINE * tokens * FARS * slots,
        ),
        name="cache_term",
    )(limits, queries, cache)
    received = lax.all_to_all(partial, "ctx", 0, 0, axis_index_groups=NEARS, tiled=True)
    gain = jnp.broadcast_to(key_gain[:, None], (head_dim, tokens))
    return pl.pallas_call(
        final_kernel,
        out_shape=jax.ShapeDtypeStruct((tokens, head_dim), jnp.bfloat16),
        in_specs=[VMEM] * 5,
        out_specs=VMEM,
        compiler_params=SMALL,
        name="final_join",
    )(own_query, received, gain, cosine, sine)


def solution(mesh):
    return jax.shard_map(
        per_device,
        mesh=mesh,
        in_specs=(
            P("req", None),
            P(None, "ctx"),
            P(None, "ctx"),
            P(None, "ctx"),
            P(),
            P(),
            P(("req", "ctx"), None),
            P(("req", "ctx"), None),
            P("req"),
            P("req"),
        ),
        out_specs=P("req", "ctx"),
        check_vma=False,
    )
```
